32 devices in a mesh: lon: 16 (over z, x, core), lat: 2 (over y).
Axes of the slice: x: 2, y: 2, z: 4, core: 2. Of those that a mesh axis runs over, the one named last changes fastest.
Arguments:
- zonal_state: float32 [4, 32, 3, 8, 2048], P(None, None, None, 'lat', 'lon'), may hold values from -6 to 6
- zonal_courant: float32 [32, 8, 2048], P(None, 'lat', 'lon'), may hold values from -0.5 to 0.5
- zonal_length: int32 [8], P('lat'), may hold values from 512 to 2048, as said below
- zonal_owner: int32 [8, 2048], P('lat', 'lon'), may hold values from 0 to 63, as said below
- merid_state: float32 [4, 32, 3, 64, 256], P(None, None, None, 'lon', 'lat'), may hold values from -6 to 6
- merid_courant: float32 [32, 64, 256], P(None, 'lon', 'lat'), may hold values from -0.5 to 0.5
- mixing: float32 [4, 32, 32], replicated, may hold values from -0.18 to 0.18
Outputs:
- zonal_next: float32 [4, 32, 3, 8, 2048], P(None, None, None, 'lat', 'lon')
- merid_next: float32 [4, 32, 3, 64, 256], P(None, None, None, 'lon', 'lat')
- coupling: float32 [64, 8, 128], P('lon', 'lat')
The draws below stay inside these ranges and needn't reach their ends.
Inputs may be any that keep to these rules, and one draw needn't show every extreme that they name: `zonal_owner`: non-decreasing along each row; each GCM column holds 16 to 48 consecutive cells of a row, and cell x belongs to a column g with |g - x // 32| <= 1. `zonal_length`: in each latitude sector (aligned blocks of 4 cycles) the first cycle holds 1088 cells and the second 2048.
All inputs are finite; a program needn't handle non-finite values.
Results may differ from the reference program's by a relative error of at most 0.0003.
Values sent between devices are 32-bit elements; how exact they have to be, the bound alone decides.
A program may use at most 64 MiB of HBM per device.

```python
import jax
import jax.numpy as jnp
from jax import lax

NV = 4
LEV = 32
WID = 3
SUB = 4
ZROWS_DEV = 4
CELLS_DEV = 128
GLON_DEV = 4
ZROWS = 8
ZCELLS = 2048
GLON = 64
MCOLS = 64
MY = 256


def draw_zonal_length(key, part):
    lengths = jax.random.randint(jax.random.fold_in(key, 5), (ZROWS,), ZCELLS // 4, ZCELLS + 1).astype(jnp.int32)
    rows = jnp.arange(ZROWS, dtype=jnp.int32)
    opposite = ZCELLS // 2 + CELLS_DEV // 2
    lengths = jnp.where(rows % ZROWS_DEV == 0, opposite, lengths)
    lengths = jnp.where(rows % ZROWS_DEV == 1, ZCELLS, lengths)
    return lengths.astype(jnp.int32)


def draw_zonal_owner(key, part):
    share = CELLS_DEV // GLON_DEV
    half = share // 2
    pairs = (GLON - 2) // 2
    shifts = jax.random.randint(jax.random.fold_in(key, 11), (ZROWS, pairs), -half, half + 1).astype(jnp.int32)
    shifts = shifts.at[0, 0].set(half)
    inner = jnp.stack([share + shifts, share - shifts], axis=-1).reshape(ZROWS, 2 * pairs)
    edge = jnp.full((ZROWS, 1), share, dtype=jnp.int32)
    widths = jnp.concatenate([edge, inner, edge], axis=1)
    ends = jnp.cumsum(widths, axis=1).astype(jnp.int32)
    cells = jnp.arange(ZCELLS, dtype=jnp.int32)

    def one_row(row_ends):
        return jnp.searchsorted(row_ends, cells, side='right').astype(jnp.int32)
    return jax.vmap(one_row)(ends).astype(jnp.int32)


def steps_of(own_key, shape, pieces, low, high):
    def one(axis_at, blocks):
        steps = jax.random.uniform(jax.random.fold_in(jax.random.fold_in(own_key, 6), axis_at), (blocks,), jnp.float32, low / len(pieces), high / len(pieces))
        return jnp.repeat(jnp.exp(steps), shape[axis_at] // blocks).reshape((-1,) + (1,) * (len(shape) - axis_at - 1))

    factor_of = one(*pieces[0])
    for cut in pieces[1:]:
        factor_of = factor_of * one(*cut)
    return factor_of


def normal_values(key, shape, deviation, bound, pieces=(), kind=jnp.bfloat16):
    entries = deviation * jax.random.normal(key, shape, jnp.float32)
    if pieces:
        entries = entries * steps_of(key, shape, pieces, -0.22, 0.18)
    return jnp.clip(entries, -bound, bound).astype(kind)


def setup_inputs(seed: int = 0) -> dict:
    key_of = jax.random.split(jax.random.key(seed), 8)
    zonal_state = normal_values(key_of[0], (NV, LEV, WID, ZROWS, ZCELLS), 1.0, 6.0, ((3, 2), (4, 16)), jnp.float32)
    zonal_courant = jnp.clip(jax.random.uniform(key_of[1], (LEV, ZROWS, ZCELLS), jnp.float32, -0.5, 0.5) * steps_of(key_of[1], (LEV, ZROWS, ZCELLS), ((1, 2), (2, 16)), -0.4, 0.0), -0.5, 0.5)
    zonal_length = draw_zonal_length(jax.random.fold_in(key_of[7], 71), 0)
    zonal_owner = draw_zonal_owner(jax.random.fold_in(key_of[7], 71), 0)
    merid_state = normal_values(key_of[4], (NV, LEV, WID, MCOLS, MY), 1.0, 6.0, ((3, 16), (4, 2)), jnp.float32)
    merid_courant = jnp.clip(jax.random.uniform(key_of[5], (LEV, MCOLS, MY), jnp.float32, -0.5, 0.5) * steps_of(key_of[5], (LEV, MCOLS, MY), ((1, 16), (2, 2)), -0.4, 0.0), -0.5, 0.5)
    mixing = normal_values(key_of[6], (NV, LEV, LEV), 0.03, 0.18, (), jnp.float32)
    return dict(zonal_state=zonal_state, zonal_courant=zonal_courant, zonal_length=zonal_length, zonal_owner=zonal_owner, merid_state=merid_state, merid_courant=merid_courant, mixing=mixing)


diffuse_along = 0.3
diffuse_across = 0.1


def across_terms(field_now):
    plus_side = jnp.concatenate([field_now[:, :, 1:], field_now[:, :, 2:3]], axis=2)
    minus_side = jnp.concatenate([field_now[:, :, 0:1], field_now[:, :, :2]], axis=2)
    return diffuse_across * (plus_side + minus_side - 2.0 * field_now)


def tendency(field_now, forward_side, backward_side, courant, mixing):
    vertical = jnp.einsum("vkj,vjwrx->vkwrx", mixing, field_now, precision=lax.Precision.HIGHEST)
    advect = -0.5 * courant * (forward_side - backward_side)
    spread = diffuse_along * (forward_side - 2.0 * field_now + backward_side)
    return advect + spread + across_terms(field_now) + vertical


def reference(zonal_state, zonal_courant, zonal_length, zonal_owner, merid_state, merid_courant, mixing):
    cells = jnp.arange(ZCELLS, dtype=jnp.int32)
    at_tail = cells[None, :] == (zonal_length[:, None] - 1)
    at_head = cells[None, :] == 0
    active = cells[None, :] < zonal_length[:, None]
    zonal_now = zonal_state
    for substep in range(SUB):
        head_cell = zonal_now[..., 0:1]
        tail_cell = jnp.sum(jnp.where(at_tail, zonal_now, 0.0), axis=-1, keepdims=True)
        forward_side = jnp.where(at_tail, head_cell, jnp.roll(zonal_now, -1, axis=-1))
        backward_side = jnp.where(at_head, tail_cell, jnp.roll(zonal_now, 1, axis=-1))
        change = tendency(zonal_now, forward_side, backward_side, zonal_courant[:, None], mixing)
        zonal_now = jnp.where(active, zonal_now + change, zonal_now)
    merid_now = merid_state
    half_turn = MCOLS // 2
    for substep in range(SUB):
        north_edge = jnp.roll(merid_now[:, :, ::-1, :, -1:], -half_turn, axis=3)
        south_edge = jnp.roll(merid_now[:, :, ::-1, :, 0:1], -half_turn, axis=3)
        forward_side = jnp.concatenate([merid_now[..., 1:], north_edge], axis=-1)
        backward_side = jnp.concatenate([south_edge, merid_now[..., :-1]], axis=-1)
        merid_now = merid_now + tendency(merid_now, forward_side, backward_side, merid_courant[:, None], mixing)
    scale = GLON_DEV / (3.0 * CELLS_DEV)
    change_sum = jnp.sum(zonal_now - zonal_state, axis=2) * scale
    flat = change_sum.reshape(NV * LEV, ZROWS, ZCELLS)
    columns = jnp.arange(GLON, dtype=jnp.int32)

    def one_row(paired):
        owner_row, change_row = paired
        onehot = (owner_row[:, None] == columns[None, :]).astype(jnp.float32)
        return jnp.einsum("xg,jx->gj", onehot, change_row, precision=lax.Precision.HIGHEST)

    rows_out = lax.map(one_row, (zonal_owner, jnp.moveaxis(flat, 1, 0)))
    coupling = jnp.transpose(rows_out, (1, 0, 2))
    return zonal_now, merid_now, coupling
```

```python
import functools

import jax
import jax.numpy as jnp
from jax import lax
from jax.experimental import pallas as pl
from jax.experimental.pallas import tpu as pltpu
from jax.sharding import PartitionSpec as P

SUB = 4
GLON_DEV = 4
PAD = 8
MESH = pl.DeviceIdType.MESH
F32 = jnp.float32


def mix_into(products, at, fields, weights):
    wide = jnp.concatenate(fields, axis=0)
    high = wide.astype(jnp.bfloat16)
    low = (wide - high.astype(F32)).astype(jnp.bfloat16)
    out = jnp.dot(jnp.concatenate([high, low], axis=1), weights[...], preferred_element_type=F32)
    half = out.shape[1] // 2
    products[pl.ds(at, wide.shape[0]), :] = out[:, :half] + out[:, half:]


def updated(now, ahead, behind, courant, product):
    c_ahead = 0.3 - 0.5 * courant
    c_behind = 0.3 + 0.5 * courant
    x0, x1, x2 = now
    local = (0.3 * x0 + 0.1 * x1, 0.2 * x1 + 0.1 * (x0 + x2), 0.3 * x2 + 0.1 * x1)
    return [
        local[w] + c_ahead * ahead[w] + c_behind * behind[w] + product[w] for w in range(3)
    ]


def substep(state, strips, products, weights, src, dst, cells, rows_dev, tails, strips_too):
    rows = 3 * cells
    for r in range(rows_dev):
        mix_into(
            products,
            r * rows,
            [state[src, w * 4 + r, pl.ds(PAD, cells), :] for w in range(3)],
            weights,
        )
    srows = 16 * rows_dev
    if strips_too:
        mix_into(
            products,
            rows_dev * rows,
            [strips[src, w, pl.ds(PAD, srows), :] for w in range(3)],
            weights,
        )
    for r in range(rows_dev):
        for w in range(3):
            edge = PAD + r * 16 + 3
            state[src, w * 4 + r, pl.ds(PAD - 1, 1), :] = strips[src, w, pl.ds(edge, 1), :]
            state[src, w * 4 + r, pl.ds(PAD + cells, 1), :] = strips[src, w, pl.ds(edge + 8, 1), :]
    step = 32
    for r in range(rows_dev):
        for at in range(0, cells, step):
            now = [state[src, w * 4 + r, pl.ds(PAD + at, step), :] for w in range(3)]
            ahead = [state[src, w * 4 + r, pl.ds(PAD + at + 1, step), :] for w in range(3)]
            behind = [state[src, w * 4 + r, pl.ds(PAD + at - 1, step), :] for w in range(3)]
            courant = state[0, 12 + r, pl.ds(PAD + at, step), :]
            product = [
                products[pl.ds(r * rows + w * cells + at, step), :] for w in range(3)
            ]
            if tails is not None:
                index = at + lax.broadcasted_iota(jnp.int32, (step, 128), 0)
                end = tails[r]
                for w in range(3):
                    beyond = strips[src, w, pl.ds(PAD + r * 16 + 11, 1), :]
                    ahead[w] = jnp.where(index == end - 1, beyond, ahead[w])
            new = updated(now, ahead, behind, courant, product)
            for w in range(3):
                value = new[w]
                if tails is not None:
                    value = jnp.where(index < end, value, now[w])
                state[dst, w * 4 + r, pl.ds(PAD + at, step), :] = value
    if strips_too:
        base = rows_dev * rows
        for at in range(0, srows, step):
            now = [strips[src, w, pl.ds(PAD + at, step), :] for w in range(3)]
            ahead = [strips[src, w, pl.ds(PAD + at + 1, step), :] for w in range(3)]
            behind = [strips[src, w, pl.ds(PAD + at - 1, step), :] for w in range(3)]
            courant = strips[0, 3, pl.ds(PAD + at, step), :]
            product = [products[pl.ds(base + w * srows + at, step), :] for w in range(3)]
            new = updated(now, ahead, behind, courant, product)
            for w in range(3):
                strips[dst, w, pl.ds(PAD + at, step), :] = new[w]


def load_state(state, field, courant, cells, rows_dev):
    for r in range(rows_dev):
        for w in range(3):
            at = w * rows_dev + r
            block = field[pl.ds(at, 128, stride=3 * rows_dev), :]
            state[0, w * 4 + r, pl.ds(PAD, cells), :] = block.T
        levels = courant[pl.ds(r, 32, stride=rows_dev), :]
        state[0, 12 + r, pl.ds(PAD, cells), :] = jnp.concatenate([levels] * 4, axis=0).T


def store_state(out, state, cells, rows_dev):
    for r in range(rows_dev):
        for w in range(3):
            at = w * rows_dev + r
            out[pl.ds(at, 128, stride=3 * rows_dev), :] = state[0, w * 4 + r, pl.ds(PAD, cells), :].T


def pack_ends(first, last, state, cells, rows_dev):
    for r in range(rows_dev):
        for ch in range(4):
            put = pl.ds((r % 2) * 4, 4)
            first[r // 2, ch, put, :] = state[0, ch * 4 + r, pl.ds(PAD, 4), :]
            last[r // 2, ch, put, :] = state[0, ch * 4 + r, pl.ds(PAD + cells - 4, 4), :]


def kernel(
    n, n_lat, cells, rows_dev,
    len_ref, z_ref, zc_ref, own_ref, m_ref, mc_ref, mix_ref,
    zo_ref, mo_ref, co_ref,
    zs, ms, zh, mh, products, weights, start_sum,
    z_first, z_last, z_tail, m_first, m_last,
    from_left, from_right, heads, tails_in, tail_zero, m_halo, head_rows,
    c_left, c_right, c_from_left, c_from_right,
    sends, recvs, tail_sends, tail_recvs, head_sends,
):
    me = lax.axis_index("lon")
    lat = lax.axis_index("lat")
    right, left = lax.rem(me + 1, n), lax.rem(me + n - 1, n)
    partner = lax.rem(me + n // 2, n)
    wrap_from = n // 4 - 1
    mid = n // 2
    start = me * cells
    barrier = pltpu.get_barrier_semaphore()

    def greet(lon_to, lat_to):
        pl.semaphore_signal(barrier, inc=1, device_id=(lon_to, lat_to), device_id_type=MESH)

    greet(left, lat)
    greet(right, lat)
    at_south, at_north = lat == 0, lat == n_lat - 1
    south_lon = jnp.where(at_south, partner, me)
    south_lat = jnp.where(at_south, 0, lat - 1)
    north_lon = jnp.where(at_north, partner, me)
    north_lat = jnp.where(at_north, n_lat - 1, lat + 1)
    greet(south_lon, south_lat)
    greet(north_lon, north_lat)

    @pl.when(me == 0)
    def _():
        for j in range(wrap_from, n):
            greet(j, lat)

    @pl.when(me >= wrap_from)
    def _():
        greet(0, lat)

    load_state(zs, z_ref, zc_ref, cells, rows_dev)
    pack_ends(z_first, z_last, zs, cells, rows_dev)
    lengths = [len_ref[r] for r in range(rows_dev)]
    index8 = lax.broadcasted_iota(jnp.int32, (8, 128), 0)
    for r in range(rows_dev):
        at = jnp.clip(lengths[r] - 4 - start, -4, cells)
        cell = lengths[r] - 4 - start + index8
        own = (cell >= 0) & (cell < cells)
        for ch in range(4):
            value = zs[0, ch * 4 + r, pl.ds(PAD + at, 8), :]
            z_tail[r // 2, ch, pl.ds((r % 2) * 4, 4), :] = jnp.where(own, value, 0.0)[:4]
    load_state(ms, m_ref, mc_ref, cells, rows_dev)
    pack_ends(m_first, m_last, ms, cells, rows_dev)

    extra = jnp.where(me == 0, n - wrap_from, jnp.where(me >= wrap_from, 1, 0))
    pl.semaphore_wait(barrier, 4 + extra)

    def copy(src, dst, send, recv, lon_to, lat_to):
        return pltpu.make_async_remote_copy(
            src_ref=src, dst_ref=dst, send_sem=send, recv_sem=recv,
            device_id=(lon_to, lat_to), device_id_type=MESH,
        )

    def head_copy(j):
        return copy(z_first.at[1], heads.at[1], head_sends.at[j], recvs.at[4], j, lat)

    head_mid = copy(z_first.at[0], heads.at[0], sends.at[5], recvs.at[5], mid, lat)
    tail_mid = copy(z_tail.at[0], tail_zero, sends.at[5], recvs.at[6], 0, lat)

    def tail_copy(j):
        return copy(z_tail.at[1], tails_in.at[j], sends.at[4], tail_recvs.at[j], 0, lat)

    @pl.when(me == 0)
    def _():
        for j in range(wrap_from, n):
            head_copy(j).start()
        head_mid.start()

    @pl.when(me >= wrap_from)
    def _():
        tail_copy(me).start()

    @pl.when(me == mid)
    def _():
        tail_mid.start()

    to_right = copy(z_last, from_left, sends.at[0], recvs.at[0], right, lat)
    to_left = copy(z_first, from_right, sends.at[1], recvs.at[1], left, lat)
    to_right.start()
    to_left.start()
    south_slot = jnp.where(at_south, 0, 1)
    north_slot = jnp.where(at_north, 1, 0)
    to_south = copy(
        m_first, m_halo.at[south_slot], sends.at[2], recvs.at[2 + south_slot], south_lon, south_lat
    )
    to_north = copy(
        m_last, m_halo.at[north_slot], sends.at[3], recvs.at[2 + north_slot], north_lon, north_lat
    )
    to_south.start()
    to_north.start()

    tiled = jnp.concatenate([mix_ref[...]] * 4, axis=1)
    block_of = lambda axis: lax.broadcasted_iota(jnp.int32, (128, 128), axis) // 32
    matrix = jnp.where(block_of(0) == block_of(1), tiled, 0.0).T
    w_high = matrix.astype(jnp.bfloat16)
    w_low = (matrix - w_high.astype(F32)).astype(jnp.bfloat16)
    pair = jnp.concatenate([w_high, w_low], axis=1)
    weights[pl.ds(0, 128), :] = pair
    weights[pl.ds(128, 128), :] = pair
    for r in range(rows_dev):
        body = pl.ds(PAD, cells)
        start_sum[r] = zs[0, r, body, :] + zs[0, 4 + r, body, :] + zs[0, 8 + r, body, :]
    for buf in (zh, mh):
        for s in range(2):
            for ch in range(4):
                buf[s, ch, pl.ds(0, 8), :] = jnp.zeros((8, 128), F32)
                buf[s, ch, pl.ds(PAD + 16 * rows_dev, 8), :] = jnp.zeros((8, 128), F32)

    to_right.wait()
    to_left.wait()

    @pl.when(me >= wrap_from)
    def _():
        tail_copy(me).wait_send()
        head_copy(me).wait_recv()

    @pl.when(me == mid)
    def _():
        tail_mid.wait_send()
        head_mid.wait_recv()

    @pl.when(me == 0)
    def _():
        for j in range(wrap_from, n):
            head_copy(j).wait_send()
            tail_copy(j).wait_recv()
        head_mid.wait_send()
        tail_mid.wait_recv()

    for r in range(rows_dev):
        take = pl.ds((r % 2) * 4, 4)
        for ch in range(4):
            zs[0, ch * 4 + r, pl.ds(PAD - 4, 4), :] = from_left[r // 2, ch, take, :]
            zs[0, ch * 4 + r, pl.ds(PAD + cells, 4), :] = from_right[r // 2, ch, take, :]

    @pl.when(me == 0)
    def _():
        for ch in range(4):
            zs[0, ch * 4, pl.ds(PAD - 4, 4), :] = tail_zero[ch, pl.ds(0, 4), :]
            total = tails_in[wrap_from, ch]
            for j in range(wrap_from + 1, n):
                total = total + tails_in[j, ch]
            for r in range(2, rows_dev):
                zs[0, ch * 4 + r, pl.ds(PAD - 4, 4), :] = total[(r % 2) * 4 : (r % 2) * 4 + 4]

    ends = []
    for r in range(rows_dev):
        room = lengths[r] - start
        end = jnp.clip(room, 0, cells)
        ends.append(end)
        over = jnp.clip(room - cells, 0, 5)
        short = jnp.clip(room, 0, 4)
        for ch in range(4):
            upper = zs[0, ch * 4 + r, pl.ds(PAD + end - 3, 8), :]
            lower = zs[0, ch * 4 + r, pl.ds(PAD - 4, 8), :]
            if r != 1:
                head_rows[r, ch, pl.ds(16, 4), :] = heads[r // 2, ch, pl.ds((r % 2) * 4, 4), :]
                upper = jnp.where(
                    index8 - 3 >= over, head_rows[r, ch, pl.ds(13 - over, 8), :], upper
                )
                lower = jnp.where(
                    index8 - 4 >= short, head_rows[r, ch, pl.ds(12 - short, 8), :], lower
                )
            zh[0, ch, pl.ds(PAD + r * 16, 8), :] = lower
            zh[0, ch, pl.ds(PAD + r * 16 + 8, 8), :] = upper

    for t in range(SUB):
        substep(
            zs, zh, products, weights, t % 2, (t + 1) % 2, cells, rows_dev, ends, t < SUB - 1
        )

    scale = GLON_DEV / (3.0 * cells)
    near = me * GLON_DEV - 1 + lax.broadcasted_iota(jnp.int32, (8, cells), 0)
    for r in range(rows_dev):
        body = pl.ds(PAD, cells)
        total = zs[0, r, body, :] + zs[0, 4 + r, body, :] + zs[0, 8 + r, body, :]
        delta = (total - start_sum[r]) * scale
        table = (own_ref[pl.ds(r, 1), :] == near).astype(F32)
        terms = jnp.dot(
            table, delta, precision=lax.Precision.HIGHEST, preferred_element_type=F32
        )
        c_left[pl.ds(r, 1), :] = terms[0:1]
        c_right[pl.ds(r, 1), :] = terms[GLON_DEV + 1 : GLON_DEV + 2]
        for g in range(GLON_DEV):
            co_ref[g, pl.ds(r, 1), :] = terms[g + 1 : g + 2]
    part_left = copy(c_left, c_from_right, sends.at[6], recvs.at[7], left, lat)
    part_right = copy(c_right, c_from_left, sends.at[7], recvs.at[8], right, lat)
    store_state(zo_ref, zs, cells, rows_dev)
    part_left.start()
    part_right.start()

    copy(m_first, m_halo.at[0], sends.at[2], recvs.at[2], south_lon, south_lat).wait()
    copy(m_last, m_halo.at[1], sends.at[3], recvs.at[3], north_lon, north_lat).wait()
    for r in range(rows_dev):
        take = (r % 2) * 4
        for ch in range(4):
            turned = ch if ch == 3 else 2 - ch
            sign = -1.0 if ch == 3 else 1.0
            base = PAD + r * 16
            for j in range(4):
                plain = m_halo[0, r // 2, ch, pl.ds(take + j, 1), :]
                pole = sign * m_halo[0, r // 2, turned, pl.ds(take + 3 - j, 1), :]
                mh[0, ch, pl.ds(base + j, 1), :] = jnp.where(at_south, pole, plain)
                plain = m_halo[1, r // 2, ch, pl.ds(take + j, 1), :]
                pole = sign * m_halo[1, r // 2, turned, pl.ds(take + 3 - j, 1), :]
                mh[0, ch, pl.ds(base + 11 + j, 1), :] = jnp.where(at_north, pole, plain)
            mh[0, ch, pl.ds(base + 4, 4), :] = ms[0, ch * 4 + r, pl.ds(PAD, 4), :]
            mh[0, ch, pl.ds(base + 8, 3), :] = ms[0, ch * 4 + r, pl.ds(PAD + cells - 3, 3), :]
            mh[0, ch, pl.ds(base + 15, 1), :] = jnp.zeros((1, 128), F32)
    for t in range(SUB):
        substep(
            ms, mh, products, weights, t % 2, (t + 1) % 2, cells, rows_dev, None, t < SUB - 1
        )
    store_state(mo_ref, ms, cells, rows_dev)
    part_left.wait()
    part_right.wait()
    for r in range(rows_dev):
        co_ref[0, pl.ds(r, 1), :] += c_from_left[pl.ds(r, 1), :]
        co_ref[GLON_DEV - 1, pl.ds(r, 1), :] += c_from_right[pl.ds(r, 1), :]


def solution(mesh):
    n, n_lat = mesh.shape["lon"], mesh.shape["lat"]

    def shards(
        zonal_state, zonal_courant, zonal_length, zonal_owner, merid_state, merid_courant, mixing
    ):
        nv, lev, wid, rows_dev, cells = zonal_state.shape
        flat = nv * lev * wid * rows_dev
        vmem = pl.BlockSpec(memory_space=pltpu.VMEM)
        state = pltpu.VMEM((2, 16, cells + 2 * PAD, 128), F32)
        strips = pltpu.VMEM((2, 4, 16 * rows_dev + 2 * PAD, 128), F32)
        packet = pltpu.VMEM((2, 4, 8, 128), F32)
        small = pltpu.VMEM((8, 128), F32)
        dma = pltpu.SemaphoreType.DMA
        zo, mo, co = pl.pallas_call(
            functools.partial(kernel, n, n_lat, cells, rows_dev),
            out_shape=(
                jax.ShapeDtypeStruct((flat, cells), F32),
                jax.ShapeDtypeStruct((flat, cells), F32),
                jax.ShapeDtypeStruct((GLON_DEV, rows_dev, nv * lev), F32),
            ),
            in_specs=[pl.BlockSpec(memory_space=pltpu.SMEM)] + [vmem] * 6,
            out_specs=(vmem, vmem, vmem),
            scratch_shapes=[
                state, state, strips, strips,
                pltpu.VMEM((rows_dev * 3 * cells + 3 * 16 * rows_dev, 128), F32),
                pltpu.VMEM((256, 256), jnp.bfloat16),
                pltpu.VMEM((rows_dev, cells, 128), F32),
                packet, packet, packet, packet, packet,
                packet, packet, packet,
                pltpu.VMEM((n, 4, 8, 128), F32),
                pltpu.VMEM((4, 8, 128), F32),
                pltpu.VMEM((2, 2, 4, 8, 128), F32),
                pltpu.VMEM((rows_dev, 4, 32, 128), F32),
                small, small, small, small,
                dma((8,)), dma((9,)), dma((1,)), dma((n,)), dma((n,)),
            ],
            compiler_params=pltpu.CompilerParams(
                collective_id=0, has_side_effects=True, vmem_limit_bytes=48 * 1024 * 1024
            ),
        )(
            zonal_length,
            zonal_state.reshape(flat, cells),
            zonal_courant.reshape(lev * rows_dev, cells),
            zonal_owner,
            merid_state.reshape(flat, cells),
            merid_courant.reshape(lev * rows_dev, cells),
            mixing.reshape(nv * lev, lev),
        )
        return zo.reshape(zonal_state.shape), mo.reshape(merid_state.shape), co

    return jax.shard_map(
        shards,
        mesh=mesh,
        in_specs=(
            P(None, None, None, "lat", "lon"),
            P(None, "lat", "lon"),
            P("lat"),
            P("lat", "lon"),
            P(None, None, None, "lon", "lat"),
            P(None, "lon", "lat"),
            P(),
        ),
        out_specs=(
            P(None, None, None, "lat", "lon"),
            P(None, None, None, "lon", "lat"),
            P("lon", "lat", None),
        ),
        check_vma=False,
    )
```

```python
import functools

import jax
import jax.numpy as jnp
from jax import lax
from jax.experimental import pallas as pl
from jax.experimental.pallas import tpu as pltpu
from jax.sharding import PartitionSpec as P

SUB = 4
GLON_DEV = 4
PAD = 8
MESH = pl.DeviceIdType.MESH
F32 = jnp.float32


def mix_into(products, at, fields, weights):
    wide = jnp.concatenate(fields, axis=0)
    high = wide.astype(jnp.bfloat16)
    low = (wide - high.astype(F32)).astype(jnp.bfloat16)
    out = jnp.dot(jnp.concatenate([high, low], axis=1), weights[...], preferred_element_type=F32)
    half = out.shape[1] // 2
    products[pl.ds(at, wide.shape[0]), :] = out[:, :half] + out[:, half:]


def updated(now, ahead, behind, courant, product):
    c_ahead = 0.3 - 0.5 * courant
    c_behind = 0.3 + 0.5 * courant
    x0, x1, x2 = now
    local = (0.3 * x0 + 0.1 * x1, 0.2 * x1 + 0.1 * (x0 + x2), 0.3 * x2 + 0.1 * x1)
    return [
        local[w] + c_ahead * ahead[w] + c_behind * behind[w] + product[w] for w in range(3)
    ]


def substep(state, strips, products, weights, src, dst, cells, rows_dev, tails, strips_too):
    rows = 3 * cells
    for r in range(rows_dev):
        mix_into(
            products,
            r * rows,
            [state[src][w * 4 + r, pl.ds(PAD, cells), :] for w in range(3)],
            weights,
        )
    srows = 16 * rows_dev
    if strips_too:
        mix_into(
            products,
            rows_dev * rows,
            [strips[src][w, pl.ds(PAD, srows), :] for w in range(3)],
            weights,
        )
    for r in range(rows_dev):
        for w in range(3):
            edge = PAD + r * 16 + 3
            state[src][w * 4 + r, pl.ds(PAD - 1, 1), :] = strips[src][w, pl.ds(edge, 1), :]
            state[src][w * 4 + r, pl.ds(PAD + cells, 1), :] = strips[src][w, pl.ds(edge + 8, 1), :]
    step = 32
    for r in range(rows_dev):
        for at in range(0, cells, step):
            now = [state[src][w * 4 + r, pl.ds(PAD + at, step), :] for w in range(3)]
            ahead = [state[src][w * 4 + r, pl.ds(PAD + at + 1, step), :] for w in range(3)]
            behind = [state[src][w * 4 + r, pl.ds(PAD + at - 1, step), :] for w in range(3)]
            courant = state[0][12 + r, pl.ds(PAD + at, step), :]
            product = [
                products[pl.ds(r * rows + w * cells + at, step), :] for w in range(3)
            ]
            if tails is not None:
                index = at + lax.broadcasted_iota(jnp.int32, (step, 128), 0)
                end = tails[r]
                for w in range(3):
                    beyond = strips[src][w, pl.ds(PAD + r * 16 + 11, 1), :]
                    ahead[w] = jnp.where(index == end - 1, beyond, ahead[w])
            new = updated(now, ahead, behind, courant, product)
            for w in range(3):
                value = new[w]
                if tails is not None:
                    value = jnp.where(index < end, value, now[w])
                state[dst][w * 4 + r, pl.ds(PAD + at, step), :] = value
    if strips_too:
        base = rows_dev * rows
        for at in range(0, srows, step):
            now = [strips[src][w, pl.ds(PAD + at, step), :] for w in range(3)]
            ahead = [strips[src][w, pl.ds(PAD + at + 1, step), :] for w in range(3)]
            behind = [strips[src][w, pl.ds(PAD + at - 1, step), :] for w in range(3)]
            courant = strips[0][3, pl.ds(PAD + at, step), :]
            product = [products[pl.ds(base + w * srows + at, step), :] for w in range(3)]
            new = updated(now, ahead, behind, courant, product)
            for w in range(3):
                strips[dst][w, pl.ds(PAD + at, step), :] = new[w]


def load_state(state, field, courant, cells, rows_dev):
    for r in range(rows_dev):
        for w in range(3):
            at = w * rows_dev + r
            block = field[pl.ds(at, 128, stride=3 * rows_dev), :]
            state[w * 4 + r, pl.ds(PAD, cells), :] = block.T
        levels = courant[pl.ds(r, 32, stride=rows_dev), :]
        state[12 + r, pl.ds(PAD, cells), :] = jnp.concatenate([levels] * 4, axis=0).T


def store_state(out, state, cells, rows_dev):
    for r in range(rows_dev):
        for w in range(3):
            at = w * rows_dev + r
            out[pl.ds(at, 128, stride=3 * rows_dev), :] = state[w * 4 + r, pl.ds(PAD, cells), :].T


def pack_ends(first, last, state, cells, rows_dev):
    for r in range(rows_dev):
        for ch in range(4):
            put = pl.ds((r % 2) * 4, 4)
            first[r // 2, ch, put, :] = state[ch * 4 + r, pl.ds(PAD, 4), :]
            last[r // 2, ch, put, :] = state[ch * 4 + r, pl.ds(PAD + cells - 4, 4), :]


def kernel(
    n, n_lat, cells, rows_dev,
    len_hbm, z_hbm, zc_hbm, own_hbm, m_hbm, mc_hbm, mix_hbm,
    zs, ms, ms1, mh, mh1, weights, co_ref,
    len_ref, z_ref, zc_ref, own_ref, m_ref, mc_ref, mix_ref, in_sems,
    zs1, zh, zh1, products, start_sum,
    z_first, z_last, z_tail, m_first, m_last,
    from_left, from_right, heads, tails_in, tail_zero, m_halo, head_rows,
    c_left, c_right, c_from_left, c_from_right,
    sends, recvs, tail_sends, tail_recvs, head_sends,
):
    me = lax.axis_index("lon")
    lat = lax.axis_index("lat")
    right, left = lax.rem(me + 1, n), lax.rem(me + n - 1, n)
    partner = lax.rem(me + n // 2, n)
    wrap_from = n // 4 - 1
    mid = n // 2
    start = me * cells
    loads = [
        pltpu.make_async_copy(src, dst, in_sems.at[i])
        for i, (src, dst) in enumerate(
            (
                (z_hbm, z_ref), (zc_hbm, zc_ref), (len_hbm, len_ref), (m_hbm, m_ref),
                (mc_hbm, mc_ref), (mix_hbm, mix_ref), (own_hbm, own_ref),
            )
        )
    ]
    for load in loads:
        load.start()
    barrier = pltpu.get_barrier_semaphore()

    def greet(lon_to, lat_to):
        pl.semaphore_signal(barrier, inc=1, device_id=(lon_to, lat_to), device_id_type=MESH)

    greet(left, lat)
    greet(right, lat)
    at_south, at_north = lat == 0, lat == n_lat - 1
    south_lon = jnp.where(at_south, partner, me)
    south_lat = jnp.where(at_south, 0, lat - 1)
    north_lon = jnp.where(at_north, partner, me)
    north_lat = jnp.where(at_north, n_lat - 1, lat + 1)
    greet(south_lon, south_lat)
    greet(north_lon, north_lat)

    @pl.when(me == 0)
    def _():
        for j in range(wrap_from, n):
            greet(j, lat)

    @pl.when(me >= wrap_from)
    def _():
        greet(0, lat)

    for load in loads[:3]:
        load.wait()
    load_state(zs, z_ref, zc_ref, cells, rows_dev)
    pack_ends(z_first, z_last, zs, cells, rows_dev)
    lengths = [len_ref[r] for r in range(rows_dev)]
    index8 = lax.broadcasted_iota(jnp.int32, (8, 128), 0)
    for r in range(rows_dev):
        at = jnp.clip(lengths[r] - 4 - start, -4, cells)
        cell = lengths[r] - 4 - start + index8
        own = (cell >= 0) & (cell < cells)
        for ch in range(4):
            value = zs[ch * 4 + r, pl.ds(PAD + at, 8), :]
            z_tail[r // 2, ch, pl.ds((r % 2) * 4, 4), :] = jnp.where(own, value, 0.0)[:4]
    extra = jnp.where(me == 0, n - wrap_from, jnp.where(me >= wrap_from, 1, 0))
    pl.semaphore_wait(barrier, 4 + extra)

    def copy(src, dst, send, recv, lon_to, lat_to):
        return pltpu.make_async_remote_copy(
            src_ref=src, dst_ref=dst, send_sem=send, recv_sem=recv,
            device_id=(lon_to, lat_to), device_id_type=MESH,
        )

    def head_copy(j):
        return copy(z_first.at[1], heads.at[1], head_sends.at[j], recvs.at[4], j, lat)

    head_mid = copy(z_first.at[0], heads.at[0], sends.at[5], recvs.at[5], mid, lat)
    tail_mid = copy(z_tail.at[0], tail_zero, sends.at[5], recvs.at[6], 0, lat)

    def tail_copy(j):
        return copy(z_tail.at[1], tails_in.at[j], sends.at[4], tail_recvs.at[j], 0, lat)

    @pl.when(me == 0)
    def _():
        for j in range(wrap_from, n):
            head_copy(j).start()
        head_mid.start()

    @pl.when(me >= wrap_from)
    def _():
        tail_copy(me).start()

    @pl.when(me == mid)
    def _():
        tail_mid.start()

    to_right = copy(z_last, from_left, sends.at[0], recvs.at[0], right, lat)
    to_left = copy(z_first, from_right, sends.at[1], recvs.at[1], left, lat)
    to_right.start()
    to_left.start()
    for load in loads[3:]:
        load.wait()
    load_state(ms, m_ref, mc_ref, cells, rows_dev)
    pack_ends(m_first, m_last, ms, cells, rows_dev)
    south_slot = jnp.where(at_south, 0, 1)
    north_slot = jnp.where(at_north, 1, 0)
    to_south = copy(
        m_first, m_halo.at[south_slot], sends.at[2], recvs.at[2 + south_slot], south_lon, south_lat
    )
    to_north = copy(
        m_last, m_halo.at[north_slot], sends.at[3], recvs.at[2 + north_slot], north_lon, north_lat
    )
    to_south.start()
    to_north.start()

    tiled = jnp.concatenate([mix_ref[...]] * 4, axis=1)
    block_of = lambda axis: lax.broadcasted_iota(jnp.int32, (128, 128), axis) // 32
    matrix = jnp.where(block_of(0) == block_of(1), tiled, 0.0).T
    w_high = matrix.astype(jnp.bfloat16)
    w_low = (matrix - w_high.astype(F32)).astype(jnp.bfloat16)
    pair = jnp.concatenate([w_high, w_low], axis=1)
    weights[pl.ds(0, 128), :] = pair
    weights[pl.ds(128, 128), :] = pair
    for r in range(rows_dev):
        body = pl.ds(PAD, cells)
        start_sum[r] = zs[r, body, :] + zs[4 + r, body, :] + zs[8 + r, body, :]
    for buf in (zh, zh1, mh, mh1):
        for ch in range(3):
            buf[ch, pl.ds(0, 8), :] = jnp.zeros((8, 128), F32)
            buf[ch, pl.ds(PAD + 16 * rows_dev, 8), :] = jnp.zeros((8, 128), F32)

    copy(m_first, m_halo.at[0], sends.at[2], recvs.at[2], south_lon, south_lat).wait()
    copy(m_last, m_halo.at[1], sends.at[3], recvs.at[3], north_lon, north_lat).wait()
    for r in range(rows_dev):
        take = (r % 2) * 4
        for ch in range(4):
            turned = ch if ch == 3 else 2 - ch
            sign = -1.0 if ch == 3 else 1.0
            base = PAD + r * 16
            for j in range(4):
                plain = m_halo[0, r // 2, ch, pl.ds(take + j, 1), :]
                pole = sign * m_halo[0, r // 2, turned, pl.ds(take + 3 - j, 1), :]
                mh[ch, pl.ds(base + j, 1), :] = jnp.where(at_south, pole, plain)
                plain = m_halo[1, r // 2, ch, pl.ds(take + j, 1), :]
                pole = sign * m_halo[1, r // 2, turned, pl.ds(take + 3 - j, 1), :]
                mh[ch, pl.ds(base + 11 + j, 1), :] = jnp.where(at_north, pole, plain)
            mh[ch, pl.ds(base + 4, 4), :] = ms[ch * 4 + r, pl.ds(PAD, 4), :]
            mh[ch, pl.ds(base + 8, 3), :] = ms[ch * 4 + r, pl.ds(PAD + cells - 3, 3), :]
            mh[ch, pl.ds(base + 15, 1), :] = jnp.zeros((1, 128), F32)
    for t in range(SUB // 2):
        substep(
            (ms, ms1), (mh, mh1), products, weights, t % 2, (t + 1) % 2, cells, rows_dev, None,
            True,
        )
    to_right.wait()
    to_left.wait()

    @pl.when(me >= wrap_from)
    def _():
        tail_copy(me).wait_send()
        head_copy(me).wait_recv()

    @pl.when(me == mid)
    def _():
        tail_mid.wait_send()
        head_mid.wait_recv()

    @pl.when(me == 0)
    def _():
        for j in range(wrap_from, n):
            head_copy(j).wait_send()
            tail_copy(j).wait_recv()
        head_mid.wait_send()
        tail_mid.wait_recv()

    for r in range(rows_dev):
        take = pl.ds((r % 2) * 4, 4)
        for ch in range(4):
            zs[ch * 4 + r, pl.ds(PAD - 4, 4), :] = from_left[r // 2, ch, take, :]
            zs[ch * 4 + r, pl.ds(PAD + cells, 4), :] = from_right[r // 2, ch, take, :]

    @pl.when(me == 0)
    def _():
        for ch in range(4):
            zs[ch * 4, pl.ds(PAD - 4, 4), :] = tail_zero[ch, pl.ds(0, 4), :]
            total = tails_in[wrap_from, ch]
            for j in range(wrap_from + 1, n):
                total = total + tails_in[j, ch]
            for r in range(2, rows_dev):
                zs[ch * 4 + r, pl.ds(PAD - 4, 4), :] = total[(r % 2) * 4 : (r % 2) * 4 + 4]

    ends = []
    for r in range(rows_dev):
        room = lengths[r] - start
        end = jnp.clip(room, 0, cells)
        ends.append(end)
        over = jnp.clip(room - cells, 0, 5)
        short = jnp.clip(room, 0, 4)
        for ch in range(4):
            upper = zs[ch * 4 + r, pl.ds(PAD + end - 3, 8), :]
            lower = zs[ch * 4 + r, pl.ds(PAD - 4, 8), :]
            if r != 1:
                head_rows[r, ch, pl.ds(16, 4), :] = heads[r // 2, ch, pl.ds((r % 2) * 4, 4), :]
                upper = jnp.where(
                    index8 - 3 >= over, head_rows[r, ch, pl.ds(13 - over, 8), :], upper
                )
                lower = jnp.where(
                    index8 - 4 >= short, head_rows[r, ch, pl.ds(12 - short, 8), :], lower
                )
            zh[ch, pl.ds(PAD + r * 16, 8), :] = lower
            zh[ch, pl.ds(PAD + r * 16 + 8, 8), :] = upper

    for t in range(SUB):
        substep(
            (zs, zs1), (zh, zh1), products, weights, t % 2, (t + 1) % 2, cells, rows_dev, ends,
            t < SUB - 1,
        )

    scale = GLON_DEV / (3.0 * cells)
    near = me * GLON_DEV - 1 + lax.broadcasted_iota(jnp.int32, (8, cells), 0)
    for r in range(rows_dev):
        body = pl.ds(PAD, cells)
        total = zs[r, body, :] + zs[4 + r, body, :] + zs[8 + r, body, :]
        delta = (total - start_sum[r]) * scale
        table = (own_ref[pl.ds(r, 1), :] == near).astype(F32)
        terms = jnp.dot(
            table, delta, precision=lax.Precision.HIGHEST, preferred_element_type=F32
        )
        c_left[pl.ds(r, 1), :] = terms[0:1]
        c_right[pl.ds(r, 1), :] = terms[GLON_DEV + 1 : GLON_DEV + 2]
        for g in range(GLON_DEV):
            co_ref[g, pl.ds(r, 1), :] = terms[g + 1 : g + 2]
    part_left = copy(c_left, c_from_right, sends.at[6], recvs.at[7], left, lat)
    part_right = copy(c_right, c_from_left, sends.at[7], recvs.at[8], right, lat)
    part_left.start()
    part_right.start()

    for t in range(SUB // 2, SUB - 1):
        substep(
            (ms, ms1), (mh, mh1), products, weights, t % 2, (t + 1) % 2, cells, rows_dev, None,
            True,
        )
    part_left.wait()
    part_right.wait()
    for r in range(rows_dev):
        co_ref[0, pl.ds(r, 1), :] += c_from_left[pl.ds(r, 1), :]
        co_ref[GLON_DEV - 1, pl.ds(r, 1), :] += c_from_right[pl.ds(r, 1), :]


def finish(
    cells, rows_dev,
    zs, ms, ms1, mh, mh1, weights, co_in,
    zo_hbm, mo_hbm, co_hbm,
    zo, mo, products, sems,
):
    co_copy = pltpu.make_async_copy(co_in, co_hbm, sems.at[2])
    co_copy.start()
    store_state(zo, zs, cells, rows_dev)
    zo_copy = pltpu.make_async_copy(zo, zo_hbm, sems.at[0])
    zo_copy.start()
    substep(
        (ms, ms1), (mh, mh1), products, weights, (SUB - 1) % 2, SUB % 2, cells, rows_dev, None, False
    )
    store_state(mo, ms, cells, rows_dev)
    mo_copy = pltpu.make_async_copy(mo, mo_hbm, sems.at[1])
    mo_copy.start()
    co_copy.wait()
    zo_copy.wait()
    mo_copy.wait()


def solution(mesh):
    n, n_lat = mesh.shape["lon"], mesh.shape["lat"]

    def shards(
        zonal_state, zonal_courant, zonal_length, zonal_owner, merid_state, merid_courant, mixing
    ):
        nv, lev, wid, rows_dev, cells = zonal_state.shape
        flat = nv * lev * wid * rows_dev
        vmem = pl.BlockSpec(memory_space=pltpu.VMEM)
        hbm = pl.BlockSpec(memory_space=pltpu.HBM)
        shape = jax.ShapeDtypeStruct
        state = (16, cells + 2 * PAD, 128)
        strips = (4, 16 * rows_dev + 2 * PAD, 128)
        packet = pltpu.VMEM((2, 4, 8, 128), F32)
        small = pltpu.VMEM((8, 128), F32)
        products = pltpu.VMEM((rows_dev * 3 * cells + 3 * 16 * rows_dev, 128), F32)
        dma = pltpu.SemaphoreType.DMA
        held = pl.pallas_call(
            functools.partial(kernel, n, n_lat, cells, rows_dev),
            out_shape=(
                shape(state, F32), shape(state, F32), shape(state, F32),
                shape(strips, F32), shape(strips, F32),
                shape((256, 256), jnp.bfloat16),
                shape((GLON_DEV, rows_dev, nv * lev), F32),
            ),
            in_specs=[hbm] * 7,
            out_specs=(vmem,) * 7,
            scratch_shapes=[
                pltpu.SMEM((rows_dev,), jnp.int32),
                pltpu.VMEM((flat, cells), F32),
                pltpu.VMEM((lev * rows_dev, cells), F32),
                pltpu.VMEM((rows_dev, cells), jnp.int32),
                pltpu.VMEM((flat, cells), F32),
                pltpu.VMEM((lev * rows_dev, cells), F32),
                pltpu.VMEM((nv * lev, lev), F32),
                dma((7,)),
                pltpu.VMEM(state, F32), pltpu.VMEM(strips, F32), pltpu.VMEM(strips, F32),
                products,
                pltpu.VMEM((rows_dev, cells, 128), F32),
                packet, packet, packet, packet, packet,
                packet, packet, packet,
                pltpu.VMEM((n, 4, 8, 128), F32),
                pltpu.VMEM((4, 8, 128), F32),
                pltpu.VMEM((2, 2, 4, 8, 128), F32),
                pltpu.VMEM((rows_dev, 4, 32, 128), F32),
                small, small, small, small,
                dma((8,)), dma((9,)), dma((1,)), dma((n,)), dma((n,)),
            ],
            compiler_params=pltpu.CompilerParams(
                collective_id=0, has_side_effects=True, vmem_limit_bytes=48 * 1024 * 1024
            ),
        )(
            *(
                pltpu.with_memory_space_constraint(value, pltpu.HBM)
                for value in (
                    zonal_length,
                    zonal_state.reshape(flat, cells),
                    zonal_courant.reshape(lev * rows_dev, cells),
                    zonal_owner,
                    merid_state.reshape(flat, cells),
                    merid_courant.reshape(lev * rows_dev, cells),
                    mixing.reshape(nv * lev, lev),
                )
            )
        )
        zo, mo, co = pl.pallas_call(
            functools.partial(finish, cells, rows_dev),
            out_shape=(
                shape((flat, cells), F32), shape((flat, cells), F32),
                shape((GLON_DEV, rows_dev, nv * lev), F32),
            ),
            in_specs=[vmem] * 7,
            out_specs=(hbm,) * 3,
            scratch_shapes=[
                pltpu.VMEM((flat, cells), F32), pltpu.VMEM((flat, cells), F32), products, dma((3,)),
            ],
            compiler_params=pltpu.CompilerParams(vmem_limit_bytes=40 * 1024 * 1024),
        )(*held)
        return zo.reshape(zonal_state.shape), mo.reshape(merid_state.shape), co

    return jax.shard_map(
        shards,
        mesh=mesh,
        in_specs=(
            P(None, None, None, "lat", "lon"),
            P(None, "lat", "lon"),
            P("lat"),
            P("lat", "lon"),
            P(None, None, None, "lon", "lat"),
            P(None, "lon", "lat"),
            P(),
        ),
        out_specs=(
            P(None, None, None, "lat", "lon"),
            P(None, None, None, "lon", "lat"),
            P("lon", "lat", None),
        ),
        check_vma=False,
    )
```

```python
import functools

import jax
import jax.numpy as jnp
from jax import lax
from jax.experimental import pallas as pl
from jax.experimental.pallas import tpu as pltpu
from jax.sharding import PartitionSpec as P

SUB = 4
GLON_DEV = 4
PAD = 8
MESH = pl.DeviceIdType.MESH
F32 = jnp.float32


def mix_into(products, at, fields, weights):
    wide = jnp.concatenate(fields, axis=0)
    high = wide.astype(jnp.bfloat16)
    low = (wide - high.astype(F32)).astype(jnp.bfloat16)
    out = jnp.dot(jnp.concatenate([high, low], axis=1), weights[...], preferred_element_type=F32)
    half = out.shape[1] // 2
    products[pl.ds(at, wide.shape[0]), :] = out[:, :half] + out[:, half:]


def updated(now, ahead, behind, courant, product):
    c_ahead = 0.3 - 0.5 * courant
    c_behind = 0.3 + 0.5 * courant
    x0, x1, x2 = now
    local = (0.3 * x0 + 0.1 * x1, 0.2 * x1 + 0.1 * (x0 + x2), 0.3 * x2 + 0.1 * x1)
    return [
        local[w] + c_ahead * ahead[w] + c_behind * behind[w] + product[w] for w in range(3)
    ]


def advance(src, dst, courants, products, weights, cells, rows_dev, ends):
    rows = 3 * cells
    step = 32
    for r in range(rows_dev):
        mix_into(
            products,
            r * rows,
            [src[w * 4 + r, pl.ds(PAD, cells), :] for w in range(3)],
            weights,
        )
    for r in range(rows_dev):
        for at in range(0, cells, step):
            now = [src[w * 4 + r, pl.ds(PAD + at, step), :] for w in range(3)]
            ahead = [src[w * 4 + r, pl.ds(PAD + at + 1, step), :] for w in range(3)]
            behind = [src[w * 4 + r, pl.ds(PAD + at - 1, step), :] for w in range(3)]
            courant = courants[12 + r, pl.ds(PAD + at, step), :]
            product = [
                products[pl.ds(r * rows + w * cells + at, step), :] for w in range(3)
            ]
            new = updated(now, ahead, behind, courant, product)
            for w in range(3):
                value = new[w]
                if ends is not None:
                    index = at + lax.broadcasted_iota(jnp.int32, (step, 128), 0)
                    value = jnp.where(index < ends[r], value, now[w])
                dst[w * 4 + r, pl.ds(PAD + at, step), :] = value


def advance_strips(first, second, products, weights, rows_dev):
    rows = 32 * rows_dev
    step = 32
    for t in range(SUB):
        src, dst = (first, second) if t % 2 == 0 else (second, first)
        mix_into(products, 0, [src[w, pl.ds(PAD, rows), :] for w in range(3)], weights)
        for at in range(0, rows, step):
            now = [src[w, pl.ds(PAD + at, step), :] for w in range(3)]
            ahead = [src[w, pl.ds(PAD + at + 1, step), :] for w in range(3)]
            behind = [src[w, pl.ds(PAD + at - 1, step), :] for w in range(3)]
            courant = first[3, pl.ds(PAD + at, step), :]
            product = [products[pl.ds(w * rows + at, step), :] for w in range(3)]
            new = updated(now, ahead, behind, courant, product)
            for w in range(3):
                dst[w, pl.ds(PAD + at, step), :] = new[w]


def load_state(state, field, courant, cells, rows_dev):
    for r in range(rows_dev):
        for w in range(3):
            at = w * rows_dev + r
            block = field[pl.ds(at, 128, stride=3 * rows_dev), :]
            state[w * 4 + r, pl.ds(PAD, cells), :] = block.T
        levels = courant[pl.ds(r, 32, stride=rows_dev), :]
        state[12 + r, pl.ds(PAD, cells), :] = jnp.concatenate([levels] * 4, axis=0).T


def store_state(out, state, cells, rows_dev):
    for r in range(rows_dev):
        for w in range(3):
            at = w * rows_dev + r
            out[pl.ds(at, 128, stride=3 * rows_dev), :] = state[w * 4 + r, pl.ds(PAD, cells), :].T


def pack_ends(first, last, state, cells, rows_dev):
    for r in range(rows_dev):
        for ch in range(4):
            put = pl.ds((r % 2) * 4, 4)
            first[r // 2, ch, put, :] = state[ch * 4 + r, pl.ds(PAD, 4), :]
            last[r // 2, ch, put, :] = state[ch * 4 + r, pl.ds(PAD + cells - 4, 4), :]


def kernel(
    n, n_lat, cells, rows_dev,
    len_hbm, z_hbm, zc_hbm, own_hbm, m_hbm, mc_hbm, mix_hbm,
    zs2, ms, ms1, mh, weights, co_ref,
    len_ref, z_ref, zc_ref, own_ref, m_ref, mc_ref, mix_ref, in_sems,
    zs, zs1, ms2, mh1, zh, zh1, products,
    z_first, z_last, z_tail, m_first, m_last,
    from_left, from_right, heads, tails_in, tail_zero, m_halo, head_rows,
    c_left, c_right, c_from_left, c_from_right,
    sends, recvs, tail_sends, tail_recvs, head_sends,
):
    me = lax.axis_index("lon")
    lat = lax.axis_index("lat")
    right, left = lax.rem(me + 1, n), lax.rem(me + n - 1, n)
    partner = lax.rem(me + n // 2, n)
    wrap_from = n // 4 - 1
    mid = n // 2
    start = me * cells
    loads = [
        pltpu.make_async_copy(src, dst, in_sems.at[i])
        for i, (src, dst) in enumerate(
            (
                (z_hbm, z_ref), (zc_hbm, zc_ref), (len_hbm, len_ref), (m_hbm, m_ref),
                (mc_hbm, mc_ref), (mix_hbm, mix_ref), (own_hbm, own_ref),
            )
        )
    ]
    for load in loads:
        load.start()
    barrier = pltpu.get_barrier_semaphore()

    def greet(lon_to, lat_to):
        pl.semaphore_signal(barrier, inc=1, device_id=(lon_to, lat_to), device_id_type=MESH)

    greet(left, lat)
    greet(right, lat)
    at_south, at_north = lat == 0, lat == n_lat - 1
    south_lon = jnp.where(at_south, partner, me)
    south_lat = jnp.where(at_south, 0, lat - 1)
    north_lon = jnp.where(at_north, partner, me)
    north_lat = jnp.where(at_north, n_lat - 1, lat + 1)
    greet(south_lon, south_lat)
    greet(north_lon, north_lat)

    @pl.when(me == 0)
    def _():
        for j in range(wrap_from, n):
            greet(j, lat)

    @pl.when(me >= wrap_from)
    def _():
        greet(0, lat)

    for load in loads[:3]:
        load.wait()
    load_state(zs, z_ref, zc_ref, cells, rows_dev)
    pack_ends(z_first, z_last, zs, cells, rows_dev)
    lengths = [len_ref[r] for r in range(rows_dev)]
    index8 = lax.broadcasted_iota(jnp.int32, (8, 128), 0)
    for r in range(rows_dev):
        at = jnp.clip(lengths[r] - 4 - start, -4, cells)
        cell = lengths[r] - 4 - start + index8
        own = (cell >= 0) & (cell < cells)
        for ch in range(4):
            value = zs[ch * 4 + r, pl.ds(PAD + at, 8), :]
            z_tail[r // 2, ch, pl.ds((r % 2) * 4, 4), :] = jnp.where(own, value, 0.0)[:4]
    extra = jnp.where(me == 0, n - wrap_from, jnp.where(me >= wrap_from, 1, 0))
    pl.semaphore_wait(barrier, 4 + extra)

    def copy(src, dst, send, recv, lon_to, lat_to):
        return pltpu.make_async_remote_copy(
            src_ref=src, dst_ref=dst, send_sem=send, recv_sem=recv,
            device_id=(lon_to, lat_to), device_id_type=MESH,
        )

    def head_copy(j):
        return copy(z_first.at[1], heads.at[1], head_sends.at[j], recvs.at[4], j, lat)

    head_mid = copy(z_first.at[0], heads.at[0], sends.at[5], recvs.at[5], mid, lat)
    tail_mid = copy(z_tail.at[0], tail_zero, sends.at[5], recvs.at[6], 0, lat)

    def tail_copy(j):
        return copy(z_tail.at[1], tails_in.at[j], sends.at[4], tail_recvs.at[j], 0, lat)

    @pl.when(me == 0)
    def _():
        for j in range(wrap_from, n):
            head_copy(j).start()
        head_mid.start()

    @pl.when(me >= wrap_from)
    def _():
        tail_copy(me).start()

    @pl.when(me == mid)
    def _():
        tail_mid.start()

    to_right = copy(z_last, from_left, sends.at[0], recvs.at[0], right, lat)
    to_left = copy(z_first, from_right, sends.at[1], recvs.at[1], left, lat)
    to_right.start()
    to_left.start()
    for load in loads[3:]:
        load.wait()
    load_state(ms, m_ref, mc_ref, cells, rows_dev)
    pack_ends(m_first, m_last, ms, cells, rows_dev)
    south_slot = jnp.where(at_south, 0, 1)
    north_slot = jnp.where(at_north, 1, 0)
    to_south = copy(
        m_first, m_halo.at[south_slot], sends.at[2], recvs.at[2 + south_slot], south_lon, south_lat
    )
    to_north = copy(
        m_last, m_halo.at[north_slot], sends.at[3], recvs.at[2 + north_slot], north_lon, north_lat
    )
    to_south.start()
    to_north.start()

    tiled = jnp.concatenate([mix_ref[...]] * 4, axis=1)
    block_of = lambda axis: lax.broadcasted_iota(jnp.int32, (128, 128), axis) // 32
    matrix = jnp.where(block_of(0) == block_of(1), tiled, 0.0).T
    w_high = matrix.astype(jnp.bfloat16)
    w_low = (matrix - w_high.astype(F32)).astype(jnp.bfloat16)
    pair = jnp.concatenate([w_high, w_low], axis=1)
    weights[pl.ds(0, 128), :] = pair
    weights[pl.ds(128, 128), :] = pair
    for buf in (zh, zh1, mh, mh1):
        for ch in range(3):
            buf[ch, pl.ds(0, 8), :] = jnp.zeros((8, 128), F32)
            buf[ch, pl.ds(PAD + 32 * rows_dev, 8), :] = jnp.zeros((8, 128), F32)

    ends = [jnp.clip(lengths[r] - start, 0, cells) for r in range(rows_dev)]
    for src, dst in ((zs, zs1), (zs1, zs2), (zs2, zs1), (zs1, zs2)):
        advance(src, dst, zs, products, weights, cells, rows_dev, ends)
    for src, dst in ((ms, ms1), (ms1, ms2)):
        advance(src, dst, ms, products, weights, cells, rows_dev, None)

    to_right.wait()
    to_left.wait()

    @pl.when(me >= wrap_from)
    def _():
        tail_copy(me).wait_send()
        head_copy(me).wait_recv()

    @pl.when(me == mid)
    def _():
        tail_mid.wait_send()
        head_mid.wait_recv()

    @pl.when(me == 0)
    def _():
        for j in range(wrap_from, n):
            head_copy(j).wait_send()
            tail_copy(j).wait_recv()
        head_mid.wait_send()
        tail_mid.wait_recv()

    for r in range(rows_dev):
        take = pl.ds((r % 2) * 4, 4)
        for ch in range(4):
            zs[ch * 4 + r, pl.ds(PAD - 4, 4), :] = from_left[r // 2, ch, take, :]
            zs[ch * 4 + r, pl.ds(PAD + cells, 4), :] = from_right[r // 2, ch, take, :]

    @pl.when(me == 0)
    def _():
        for ch in range(4):
            zs[ch * 4, pl.ds(PAD - 4, 4), :] = tail_zero[ch, pl.ds(0, 4), :]
            total = tails_in[wrap_from, ch]
            for j in range(wrap_from + 1, n):
                total = total + tails_in[j, ch]
            for r in range(2, rows_dev):
                zs[ch * 4 + r, pl.ds(PAD - 4, 4), :] = total[(r % 2) * 4 : (r % 2) * 4 + 4]

    index16 = lax.broadcasted_iota(jnp.int32, (16, 128), 0)
    for r in range(rows_dev):
        room = lengths[r] - start
        end = ends[r]
        over = jnp.clip(room - cells, 0, 5)
        short = jnp.clip(room, 0, 12)
        for ch in range(4):
            upper = zs[ch * 4 + r, pl.ds(PAD + end - 8, 16), :]
            lower = zs[ch * 4 + r, pl.ds(PAD - 4, 16), :]
            if r != 1:
                head_rows[r, ch, pl.ds(16, 4), :] = heads[r // 2, ch, pl.ds((r % 2) * 4, 4), :]
                upper = jnp.where(
                    index16 - 8 >= over, head_rows[r, ch, pl.ds(8 - over, 16), :], upper
                )
                lower = jnp.where(
                    index16 - 4 >= short, head_rows[r, ch, pl.ds(12 - short, 16), :], lower
                )
            zh[ch, pl.ds(PAD + r * 32, 16), :] = lower
            zh[ch, pl.ds(PAD + r * 32 + 16, 16), :] = upper
    advance_strips(zh, zh1, products, weights, rows_dev)
    index4 = lax.broadcasted_iota(jnp.int32, (4, 128), 0)
    for r in range(rows_dev):
        base = PAD + r * 32
        for w in range(3):
            at = w * 4 + r
            low = zs2[at, pl.ds(PAD, 4), :]
            zs2[at, pl.ds(PAD, 4), :] = jnp.where(
                index4 < ends[r], zh[w, pl.ds(base + 4, 4), :], low
            )
        for block in range(0, cells, 8):
            ahead = block - ends[r]
            inside = (index8 + ahead >= -4) & (index8 + ahead < 0)
            take = base + 16 + jnp.clip(ahead + 8, -8, 8)
            for w in range(3):
                at = w * 4 + r
                high = zs2[at, pl.ds(PAD + block, 8), :]
                zs2[at, pl.ds(PAD + block, 8), :] = jnp.where(
                    inside, zh[w, pl.ds(take, 8), :], high
                )

    scale = GLON_DEV / (3.0 * cells)
    near = me * GLON_DEV - 1 + lax.broadcasted_iota(jnp.int32, (8, cells), 0)
    for r in range(rows_dev):
        body = pl.ds(PAD, cells)
        before = zs[r, body, :] + zs[4 + r, body, :] + zs[8 + r, body, :]
        after = zs2[r, body, :] + zs2[4 + r, body, :] + zs2[8 + r, body, :]
        delta = (after - before) * scale
        table = (own_ref[pl.ds(r, 1), :] == near).astype(F32)
        terms = jnp.dot(
            table, delta, precision=lax.Precision.HIGHEST, preferred_element_type=F32
        )
        c_left[pl.ds(r, 1), :] = terms[0:1]
        c_right[pl.ds(r, 1), :] = terms[GLON_DEV + 1 : GLON_DEV + 2]
        for g in range(GLON_DEV):
            co_ref[g, pl.ds(r, 1), :] = terms[g + 1 : g + 2]
    part_left = copy(c_left, c_from_right, sends.at[6], recvs.at[7], left, lat)
    part_right = copy(c_right, c_from_left, sends.at[7], recvs.at[8], right, lat)
    part_left.start()
    part_right.start()


    copy(m_first, m_halo.at[0], sends.at[2], recvs.at[2], south_lon, south_lat).wait()
    copy(m_last, m_halo.at[1], sends.at[3], recvs.at[3], north_lon, north_lat).wait()
    for r in range(rows_dev):
        take = (r % 2) * 4
        for ch in range(4):
            turned = ch if ch == 3 else 2 - ch
            sign = -1.0 if ch == 3 else 1.0
            base = PAD + r * 32
            for j in range(4):
                plain = m_halo[0, r // 2, ch, pl.ds(take + j, 1), :]
                pole = sign * m_halo[0, r // 2, turned, pl.ds(take + 3 - j, 1), :]
                mh[ch, pl.ds(base + j, 1), :] = jnp.where(at_south, pole, plain)
                plain = m_halo[1, r // 2, ch, pl.ds(take + j, 1), :]
                pole = sign * m_halo[1, r // 2, turned, pl.ds(take + 3 - j, 1), :]
                mh[ch, pl.ds(base + 24 + j, 1), :] = jnp.where(at_north, pole, plain)
            mh[ch, pl.ds(base + 4, 12), :] = ms[ch * 4 + r, pl.ds(PAD, 12), :]
            mh[ch, pl.ds(base + 16, 8), :] = ms[ch * 4 + r, pl.ds(PAD + cells - 8, 8), :]
            mh[ch, pl.ds(base + 28, 4), :] = jnp.zeros((4, 128), F32)
    advance_strips(mh, mh1, products, weights, rows_dev)
    advance(ms2, ms1, ms, products, weights, cells, rows_dev, None)
    part_left.wait()
    part_right.wait()
    for r in range(rows_dev):
        co_ref[0, pl.ds(r, 1), :] += c_from_left[pl.ds(r, 1), :]
        co_ref[GLON_DEV - 1, pl.ds(r, 1), :] += c_from_right[pl.ds(r, 1), :]


def finish(
    cells, rows_dev,
    zs, ms, ms1, mh, weights, co_in,
    zo_hbm, mo_hbm, co_hbm,
    zo, mo, ms2, products, sems,
):
    co_copy = pltpu.make_async_copy(co_in, co_hbm, sems.at[2])
    co_copy.start()
    store_state(zo, zs, cells, rows_dev)
    zo_copy = pltpu.make_async_copy(zo, zo_hbm, sems.at[0])
    zo_copy.start()
    advance(ms1, ms2, ms, products, weights, cells, rows_dev, None)
    for r in range(rows_dev):
        for w in range(3):
            at, base = w * 4 + r, PAD + r * 32
            ms2[at, pl.ds(PAD, 4), :] = mh[w, pl.ds(base + 4, 4), :]
            ms2[at, pl.ds(PAD + cells - 4, 4), :] = mh[w, pl.ds(base + 20, 4), :]
    store_state(mo, ms2, cells, rows_dev)
    mo_copy = pltpu.make_async_copy(mo, mo_hbm, sems.at[1])
    mo_copy.start()
    co_copy.wait()
    zo_copy.wait()
    mo_copy.wait()


def solution(mesh):
    n, n_lat = mesh.shape["lon"], mesh.shape["lat"]

    def shards(
        zonal_state, zonal_courant, zonal_length, zonal_owner, merid_state, merid_courant, mixing
    ):
        nv, lev, wid, rows_dev, cells = zonal_state.shape
        flat = nv * lev * wid * rows_dev
        vmem = pl.BlockSpec(memory_space=pltpu.VMEM)
        hbm = pl.BlockSpec(memory_space=pltpu.HBM)
        shape = jax.ShapeDtypeStruct
        state = (16, cells + 2 * PAD, 128)
        strips = (4, 32 * rows_dev + 2 * PAD, 128)
        packet = pltpu.VMEM((2, 4, 8, 128), F32)
        small = pltpu.VMEM((8, 128), F32)
        products = pltpu.VMEM((rows_dev * 3 * cells, 128), F32)
        dma = pltpu.SemaphoreType.DMA
        held = pl.pallas_call(
            functools.partial(kernel, n, n_lat, cells, rows_dev),
            out_shape=(
                shape(state, F32), shape(state, F32), shape(state, F32),
                shape(strips, F32),
                shape((256, 256), jnp.bfloat16),
                shape((GLON_DEV, rows_dev, nv * lev), F32),
            ),
            in_specs=[hbm] * 7,
            out_specs=(vmem,) * 6,
            scratch_shapes=[
                pltpu.SMEM((rows_dev,), jnp.int32),
                pltpu.VMEM((flat, cells), F32),
                pltpu.VMEM((lev * rows_dev, cells), F32),
                pltpu.VMEM((rows_dev, cells), jnp.int32),
                pltpu.VMEM((flat, cells), F32),
                pltpu.VMEM((lev * rows_dev, cells), F32),
                pltpu.VMEM((nv * lev, lev), F32),
                dma((7,)),
                pltpu.VMEM(state, F32), pltpu.VMEM(state, F32), pltpu.VMEM(state, F32),
                pltpu.VMEM(strips, F32), pltpu.VMEM(strips, F32), pltpu.VMEM(strips, F32),
                products,
                packet, packet, packet, packet, packet,
                packet, packet, packet,
                pltpu.VMEM((n, 4, 8, 128), F32),
                pltpu.VMEM((4, 8, 128), F32),
                pltpu.VMEM((2, 2, 4, 8, 128), F32),
                pltpu.VMEM((rows_dev, 4, 40, 128), F32),
                small, small, small, small,
                dma((8,)), dma((9,)), dma((1,)), dma((n,)), dma((n,)),
            ],
            compiler_params=pltpu.CompilerParams(
                collective_id=0, has_side_effects=True, vmem_limit_bytes=48 * 1024 * 1024
            ),
        )(
            *(
                pltpu.with_memory_space_constraint(value, pltpu.HBM)
                for value in (
                    zonal_length,
                    zonal_state.reshape(flat, cells),
                    zonal_courant.reshape(lev * rows_dev, cells),
                    zonal_owner,
                    merid_state.reshape(flat, cells),
                    merid_courant.reshape(lev * rows_dev, cells),
                    mixing.reshape(nv * lev, lev),
                )
            )
        )
        zo, mo, co = pl.pallas_call(
            functools.partial(finish, cells, rows_dev),
            out_shape=(
                shape((flat, cells), F32), shape((flat, cells), F32),
                shape((GLON_DEV, rows_dev, nv * lev), F32),
            ),
            in_specs=[vmem] * 6,
            out_specs=(hbm,) * 3,
            scratch_shapes=[
                pltpu.VMEM((flat, cells), F32), pltpu.VMEM((flat, cells), F32),
                pltpu.VMEM(state, F32), products, dma((3,)),
            ],
            compiler_params=pltpu.CompilerParams(vmem_limit_bytes=40 * 1024 * 1024),
        )(*held)
        return zo.reshape(zonal_state.shape), mo.reshape(merid_state.shape), co

    return jax.shard_map(
        shards,
        mesh=mesh,
        in_specs=(
            P(None, None, None, "lat", "lon"),
            P(None, "lat", "lon"),
            P("lat"),
            P("lat", "lon"),
            P(None, None, None, "lon", "lat"),
            P(None, "lon", "lat"),
            P(),
        ),
        out_specs=(
            P(None, None, None, "lat", "lon"),
            P(None, None, None, "lon", "lat"),
            P("lon", "lat", None),
        ),
        check_vma=False,
    )
```
